32 devices in a mesh: groups: 2 (over y), src: 4 (over z), tgt: 2 (over x), ill: 2 (over core).
Axes of the slice: x: 2, y: 2, z: 4, core: 2. Of those that a mesh axis runs over, the one named last changes fastest.
Arguments:
- coeffs: bfloat16 [2, 64, 8, 8, 512], P(None, ('groups', 'ill'), 'src', 'tgt'), parts along dimension 1, may hold values from -6 to 6
- reflection: float32 [2, 16, 8, 512], P(None, ('groups', 'src'), 'tgt'), parts along dimension 1, may hold values from -4.2 to 4.2
- interp: float32 [2, 3, 2, 2, 3, 8, 8], replicated, may hold values from -1 to 1
- orders: int32 [512], replicated, may hold values from 0 to 511, each once
Outputs:
- far_field: bfloat16 [2, 64, 8, 8, 512], P(None, ('groups', 'ill'), 'src', 'tgt'), parts along dimension 1
The draws below stay inside these ranges and needn't reach their ends.
There are 2 independent parts, one for each index of `groups`. The reference program is written for one: setup_inputs(seed, part) draws one part's arguments, and reference() takes and returns one part's arrays. A program takes and returns all parts, laid end to end along the dimension named above; an argument that names none is the same for every part. Nothing has to cross between parts.
Inputs may be any that keep to these rules, and one draw needn't show every extreme that they name: `orders`: each number below 512 appears exactly once.
All inputs are finite; a program needn't handle non-finite values.
Results may differ from the reference program's by a relative error of at most 0.028.
Values may be sent and summed in bfloat16 or wider, within the bound.
No kernel may reach another device: no remote copies, remote signals or barrier semaphores. Data moves between devices by JAX's collectives and lax.ppermute only.
A program may use at most 64 MiB of HBM per device.

```python
import math
import jax
import jax.numpy as jnp
from jax import lax

ORDER = 8
K = 512
LEVELS = 3
ILLUM = 32
NU = 8
NV = 8


factor_scale = 0.8908987181403393


def draw_interp(key, part):
    matrix_count = 2 * LEVELS * 2 * 2 * 3
    vectors = jax.random.normal(key, (matrix_count, ORDER, ORDER), jnp.float32)
    identity = jnp.eye(ORDER, dtype=jnp.float32)
    result = jnp.broadcast_to(identity, (matrix_count, ORDER, ORDER))
    for turn_index in range(ORDER):
        column = vectors[:, turn_index, :]
        lengths = jnp.sum(column * column, axis=-1) + 1e-06
        reflector = identity[None, :, :] - 2.0 * column[:, :, None] * column[:, None, :] / lengths[:, None, None]
        result = jnp.einsum('nij,njk->nik', result, reflector, precision=lax.Precision.HIGHEST)
    result = result * factor_scale
    return result.reshape(2, LEVELS, 2, 2, 3, ORDER, ORDER).astype(jnp.float32)


def level_of(stream_key, shape, split, smallest, top_value):
    loudness, own = 1.0, jax.random.fold_in(stream_key, 6)
    for dim, blocks in split:
        steps = jnp.exp(jax.random.uniform(jax.random.fold_in(own, dim), (blocks,), jnp.float32, smallest / len(split), top_value / len(split)))
        loudness = loudness * jnp.repeat(steps, shape[dim] // blocks).reshape([-1 if axis == dim else 1 for axis in range(len(shape))])
    return loudness


def scatter_about(key, shape, deviation, most, cuts=(), held_as=jnp.bfloat16):
    entries = deviation * jax.random.normal(key, shape, jnp.float32)
    if cuts:
        entries = entries * level_of(key, shape, cuts, -0.22, 0.18)
    return jnp.clip(entries, -most, most).astype(held_as)


def setup_inputs(seed: int = 0, part: int = 0) -> dict:
    key_of = jax.random.split(jax.random.key(seed), 5)
    part_keys = jax.random.split(jax.random.fold_in(key_of[4], part), 5)
    return {
        "coeffs": scatter_about(part_keys[0], (2, ILLUM, NU, NV, K), 1.0, 6.0, ((1, 2), (2, 4), (3, 2))),
        "reflection": scatter_about(part_keys[1], (2, NU, NV, K), 0.7, 4.2, ((1, 4), (2, 2)), jnp.float32),
        "interp": draw_interp(jax.random.fold_in(key_of[4], 71), part),
        "orders": jax.random.permutation(key_of[3], K).astype(jnp.int32),
    }


PHASE_RATE = 0.3
ALONG_SECOND = 1.7
DIRECTIONS = ((0.6, 0.48, 0.64), (-0.36, 0.8, 0.48))


def node_value(digits, order_count):
    return jnp.cos(math.pi * (2.0 * digits.astype(jnp.float32) + 1.0) / (2.0 * order_count))


def node_products(orders, operator_index, order_count):
    square = order_count * order_count
    digit_first = orders // square
    digit_second = (orders // order_count) % order_count
    digit_third = orders % order_count
    direction = DIRECTIONS[operator_index]
    summed = direction[0] * node_value(digit_first, order_count)
    summed = summed + direction[1] * node_value(digit_second, order_count)
    return summed + direction[2] * node_value(digit_third, order_count)


def phase_table(products, level_index, u_positions, v_positions):
    position = (u_positions[:, None] + 0.5) + ALONG_SECOND * (v_positions[None, :] + 0.5)
    angle_table = (PHASE_RATE * (level_index + 1)) * position[:, :, None] * products[None, None, :]
    return jnp.cos(angle_table).astype(jnp.bfloat16), jnp.sin(angle_table).astype(jnp.bfloat16)


def modulate(current, cos_part, sin_part):
    real_part = current[0].astype(jnp.float32)
    imag_part = current[1].astype(jnp.float32)
    cos_value = cos_part.astype(jnp.float32)
    sin_value = sin_part.astype(jnp.float32)
    return jnp.stack([cos_value * real_part - sin_value * imag_part,
                      cos_value * imag_part + sin_value * real_part]).astype(jnp.bfloat16)


def reflect(current, reflection):
    real_part = current[0].astype(jnp.float32)
    imag_part = current[1].astype(jnp.float32)
    return jnp.stack([reflection[0] * real_part - reflection[1] * imag_part,
                      reflection[0] * imag_part + reflection[1] * real_part]).astype(jnp.bfloat16)


def dense_transposed(factors):
    order_count = factors.shape[-1]
    coef_count = order_count ** 3
    columns = jnp.arange(coef_count, dtype=jnp.int32)
    digit_list = (columns // (order_count * order_count), (columns // order_count) % order_count,
                  columns % order_count)
    point_index = jnp.arange(order_count, dtype=jnp.int32)
    spread = []
    for dim_index in range(3):
        selector = (point_index[:, None] == digit_list[dim_index][None, :]).astype(factors.dtype)
        spread.append(jnp.dot(factors[dim_index].T, selector, precision=lax.Precision.HIGHEST))
    full_table = spread[0][:, None, None, :] * spread[1][None, :, None, :]
    full_table = full_table * spread[2][None, None, :, :]
    return full_table.reshape(coef_count, coef_count).astype(jnp.bfloat16)


def pair_level(current, products, factors, level_index, box_axis, pair_bit, u_positions, v_positions):
    cos_part, sin_part = phase_table(products, level_index, u_positions, v_positions)
    modulated = modulate(current, cos_part, sin_part)
    full_shape = modulated.shape
    coef_count = full_shape[-1]
    half_span = 2 ** pair_bit
    split_shape = full_shape[:box_axis] + (full_shape[box_axis] // (2 * half_span), 2, half_span) + full_shape[box_axis + 1:]
    halves = modulated.reshape(split_shape)
    lower_half = jnp.take(halves, 0, axis=box_axis + 1)
    upper_half = jnp.take(halves, 1, axis=box_axis + 1)
    outputs = []
    for side_index in range(2):
        lower_matrix = dense_transposed(factors[side_index, 0])
        upper_matrix = dense_transposed(factors[side_index, 1])
        summed = jnp.dot(lower_half.reshape(-1, coef_count), lower_matrix, preferred_element_type=jnp.float32)
        summed = summed + jnp.dot(upper_half.reshape(-1, coef_count), upper_matrix, preferred_element_type=jnp.float32)
        outputs.append(summed.reshape(lower_half.shape))
    combined = jnp.stack(outputs, axis=box_axis + 1).reshape(full_shape)
    return combined.astype(jnp.bfloat16)


def reference(coeffs, reflection, interp, orders):
    order_count = interp.shape[-1]
    u_positions = jnp.arange(NU, dtype=jnp.int32).astype(jnp.float32)
    v_positions = jnp.arange(NV, dtype=jnp.int32).astype(jnp.float32)
    current = coeffs
    for operator_index, box_axis, extent in ((0, 2, NU), (1, 3, NV)):
        products = node_products(orders, operator_index, order_count)
        top_bit = extent.bit_length() - 2
        for level_index in range(LEVELS):
            current = pair_level(current, products, interp[operator_index, level_index], level_index,
                                 box_axis, top_bit - level_index, u_positions, v_positions)
        if operator_index == 0:
            current = reflect(current, reflection)
    return current
```

```python
import functools
import math

import jax
import jax.numpy as jnp
from jax import lax
from jax.experimental import pallas as pl
from jax.experimental.pallas import tpu as pltpu
from jax.sharding import PartitionSpec as P

PHASE_RATE = 0.3
ALONG_SECOND = 1.7
DIRECTIONS = ((0.6, 0.48, 0.64), (-0.36, 0.8, 0.48))
F32 = jnp.float32
BF16 = jnp.bfloat16


def partner_2(value, axis, bit):
    mask = 2**bit
    pairs = [(source, source ^ mask) for source in range(lax.axis_size(axis))]
    return lax.ppermute(value, axis, pairs)


def node_value(digits, order_count):
    return jnp.cos(math.pi * (2.0 * digits.astype(F32) + 1.0) / (2.0 * order_count))


def node_products(orders, operator_index, order_count):
    square = order_count * order_count
    direction = DIRECTIONS[operator_index]
    summed = direction[0] * node_value(orders // square, order_count)
    summed = summed + direction[1] * node_value(orders // order_count % order_count, order_count)
    return summed + direction[2] * node_value(orders % order_count, order_count)


def plan_levels(level_count, extents, locals_):
    levels = []
    for operator in range(2):
        top = extents[operator].bit_length() - 2
        local_bits = locals_[operator].bit_length() - 1
        for level in range(level_count):
            bit = top - level
            if bit >= local_bits:
                levels.append((operator, level, ("src", "tgt")[operator], bit - local_bits))
            else:
                levels.append((operator, level, None, bit))
    return levels


def build_body(which_ref, spread_ref, w_ref):
    order_count = spread_ref.shape[2]
    first, second, third = spread_ref[0, 0], spread_ref[0, 1], spread_ref[0, 2]
    square = order_count * order_count
    for x in range(order_count):
        lead = first[x : x + 1] * second
        for y in range(0, order_count, 2):
            rows = jnp.concatenate([lead[y : y + 1] * third, lead[y + 1 : y + 2] * third])
            w_ref[0, x * square + y * order_count : x * square + (y + 2) * order_count] = rows.astype(BF16)


def build_matrices(spread, which):
    count = which.shape[0]
    _, dims, order_count, coef_count = spread.shape
    return pl.pallas_call(
        build_body,
        grid_spec=pltpu.PrefetchScalarGridSpec(
            num_scalar_prefetch=1,
            grid=(count,),
            in_specs=[pl.BlockSpec((1, dims, order_count, coef_count), lambda m, w: (w[m], 0, 0, 0))],
            out_specs=pl.BlockSpec((1, coef_count, coef_count), lambda m, w: (m, 0, 0)),
        ),
        out_shape=jax.ShapeDtypeStruct((count, coef_count, coef_count), BF16),
        compiler_params=pltpu.CompilerParams(vmem_limit_bytes=8 * 1024 * 1024),
        cost_estimate=pl.CostEstimate(
            flops=count * 2 * coef_count * coef_count, bytes_accessed=count * 2 * coef_count * coef_count, transcendentals=0
        ),
        name="build_matrices",
    )(which, spread)


def modulate(src, table, index, dst, boxes, ill, place):
    half = boxes * ill
    for box in range(boxes):
        real = src[box * ill : (box + 1) * ill].astype(F32)
        imag = src[half + box * ill : half + (box + 1) * ill].astype(F32)
        cos = table[index, 0, box : box + 1]
        sin = table[index, 1, box : box + 1]
        dst[place(0, box)] = (cos * real - sin * imag).astype(BF16)
        dst[place(1, box)] = (cos * imag + sin * real).astype(BF16)


def straight(boxes, ill):
    half = boxes * ill
    return lambda part, box: pl.ds(part * half + box * ill, ill)


def dot(a, b):
    return jnp.dot(a, b, preferred_element_type=F32)


def own_body(shape, index, raw, x_ref, table_ref, w_ref, out_ref, mod_ref):
    boxes, ill = shape
    if raw:
        modulate(x_ref, table_ref, index, mod_ref, boxes, ill, straight(boxes, ill))
        out_ref[...] = dot(mod_ref[...], w_ref[...])
    else:
        out_ref[...] = dot(x_ref[...], w_ref[...])


def rest_body(shape, partner_index, pairs, send_index, *refs):
    boxes_u, boxes_v, ill = shape
    boxes = boxes_u * boxes_v
    half = boxes * ill
    part_ref, got_ref, table_ref, w_ref = refs[:4]
    pair_refs = refs[4 : 4 + len(pairs)]
    out_ref, state_ref, mod_ref = refs[4 + len(pairs) :]
    if partner_index is None:
        got = got_ref[...]
    else:
        modulate(got_ref, table_ref, partner_index, mod_ref, boxes, ill, straight(boxes, ill))
        got = mod_ref[...]
    state_ref[...] = part_ref[...] + dot(got, w_ref[...])
    for number, (index, operator, bit) in enumerate(pairs):
        w4_ref = pair_refs[number]
        box_bit = bit + (boxes_v.bit_length() - 1 if operator == 0 else 0)
        low_mask = (1 << box_bit) - 1

        def place(part, box):
            side = box >> box_bit & 1
            rank = (box >> (box_bit + 1) << box_bit) | (box & low_mask)
            return pl.ds(side * half + part * (half // 2) + rank * ill, ill)

        modulate(state_ref, table_ref, index, mod_ref, boxes, ill, place)
        for side in range(2):
            result = dot(mod_ref[:half], w4_ref[2 * side]) + dot(mod_ref[half:], w4_ref[2 * side + 1])
            for part in range(2):
                for box in range(boxes):
                    if box >> box_bit & 1 == side:
                        begin = place(part, box).start - side * half
                        state_ref[straight(boxes, ill)(part, box)] = result[begin : begin + ill]
    if send_index is None:
        out_ref[...] = state_ref[...].astype(BF16)
    else:
        modulate(state_ref, table_ref, send_index, out_ref, boxes, ill, straight(boxes, ill))


def call(body, outs, scratch, flops, moved, name, *args):
    return pl.pallas_call(
        body,
        out_shape=outs,
        in_specs=[pl.BlockSpec(memory_space=pltpu.VMEM)] * len(args),
        out_specs=pl.BlockSpec(memory_space=pltpu.VMEM),
        scratch_shapes=scratch,
        compiler_params=pltpu.CompilerParams(vmem_limit_bytes=24 * 1024 * 1024),
        cost_estimate=pl.CostEstimate(flops=flops, bytes_accessed=moved, transcendentals=0),
        name=name,
    )(*args)


def on_device(coeffs, reflection, interp, orders):
    level_count = interp.shape[1]
    order_count = interp.shape[-1]
    _, ill, boxes_u, boxes_v, coef_count = coeffs.shape
    boxes = boxes_u * boxes_v
    rows = 2 * boxes * ill
    extents = (boxes_u * lax.axis_size("src"), boxes_v * lax.axis_size("tgt"))
    levels = plan_levels(level_count, extents, (boxes_u, boxes_v))
    assert levels[0][2] is not None

    partner_raw = partner_2(coeffs, levels[0][2], levels[0][3])

    place = {"src": lax.axis_index("src"), "tgt": lax.axis_index("tgt")}

    def positions(src, tgt):
        u = (src * boxes_u + jnp.arange(boxes_u, dtype=jnp.int32)).astype(F32)
        v = (tgt * boxes_v + jnp.arange(boxes_v, dtype=jnp.int32)).astype(F32)
        return (u[:, None] + 0.5 + ALONG_SECOND * (v[None, :] + 0.5)).reshape(boxes)

    own_position = positions(place["src"], place["tgt"])
    other_position = positions(place["src"] ^ 2 ** levels[0][3], place["tgt"])
    products = [node_products(orders, operator, order_count) for operator in range(2)]
    scales = jnp.stack(
        [PHASE_RATE * (level + 1) * own_position for _, level, _, _ in levels] + [PHASE_RATE * other_position]
    )
    by_level = jnp.stack([products[operator] for operator, _, _, _ in levels] + [products[0]])
    angles = scales[:, :, None] * by_level[:, None, :]
    cos = jnp.cos(angles).astype(BF16).astype(F32)
    sin = jnp.sin(angles).astype(BF16).astype(F32)
    reflect = reflection.reshape(2, boxes, coef_count)
    first = next(i for i, level in enumerate(levels) if level[0] == 1)
    mark = (jnp.arange(len(levels) + 1) == first)[:, None, None]
    table = jnp.stack(
        [
            jnp.where(mark, cos * reflect[0] - sin * reflect[1], cos),
            jnp.where(mark, cos * reflect[1] + sin * reflect[0], sin),
        ],
        axis=1,
    )

    columns = jnp.arange(coef_count, dtype=jnp.int32)
    digits = (columns // (order_count * order_count), columns // order_count % order_count, columns % order_count)
    points = jnp.arange(order_count, dtype=jnp.int32)
    factors = interp.reshape(-1, 3, order_count, order_count)
    spread = jnp.stack(
        [
            lax.dot_general(
                factors[:, d],
                (points[:, None] == digits[d][None, :]).astype(F32),
                (((1,), (0,)), ((), ())),
                precision=lax.Precision.HIGHEST,
            )
            for d in range(3)
        ],
        axis=1,
    )
    which, offset = [], []
    for operator, level, axis, bit in levels:
        base = (operator * level_count + level) * 4
        offset.append(len(which))
        if axis is None:
            which += [base, base + 1, base + 2, base + 3]
        else:
            own = lax.axis_index(axis) >> bit & 1
            which += [base + 3 * own, base + 2 * own + (1 - own)]
    which = jnp.stack([jnp.asarray(w, jnp.int32) for w in which])
    matrices = build_matrices(spread, which)

    def rowwise(value):
        return value.transpose(0, 2, 3, 1, 4).reshape(rows, coef_count)

    product_flops = 2 * rows * coef_count * coef_count
    swaps = [i for i, level in enumerate(levels) if level[2] is not None]
    current, partner = rowwise(coeffs), None
    for number, index in enumerate(swaps):
        _, _, axis, bit = levels[index]
        raw = number == 0
        partner = rowwise(partner_raw) if raw else partner_2(current, axis, bit)
        own = call(
            functools.partial(own_body, (boxes, ill), index, raw),
            jax.ShapeDtypeStruct((rows, coef_count), F32),
            [pltpu.VMEM((rows, coef_count), BF16)],
            product_flops,
            rows * coef_count * 6 + coef_count * coef_count * 2,
            f"own_{index}",
            current,
            table,
            matrices[offset[index]],
        )
        after = swaps[number + 1] if number + 1 < len(swaps) else len(levels)
        pairs = [(i, levels[i][0], levels[i][3]) for i in range(index + 1, after)]
        current = call(
            functools.partial(
                rest_body,
                (boxes_u, boxes_v, ill),
                len(levels) if raw else None,
                pairs,
                after if after < len(levels) else None,
            ),
            jax.ShapeDtypeStruct((rows, coef_count), BF16),
            [pltpu.VMEM((rows, coef_count), F32), pltpu.VMEM((rows, coef_count), BF16)],
            product_flops * (1 + 2 * len(pairs)),
            rows * coef_count * 8 + coef_count * coef_count * 2 * (1 + 4 * len(pairs)),
            f"rest_{index}",
            own,
            partner,
            table,
            matrices[offset[index] + 1],
            *[matrices[offset[i] : offset[i] + 4] for i, _, _ in pairs],
        )
    return current.reshape(2, boxes_u, boxes_v, ill, coef_count).transpose(0, 3, 1, 2, 4)


def solution(mesh):
    in_specs = (
        P(None, ("groups", "ill"), "src", "tgt", None),
        P(None, ("groups", "src"), "tgt", None),
        P(),
        P(),
    )
    out_specs = P(None, ("groups", "ill"), "src", "tgt", None)
    return jax.shard_map(
        on_device, mesh=mesh, in_specs=in_specs, out_specs=out_specs, check_vma=False
    )
```

```python
import functools
import math

import jax
import jax.numpy as jnp
from jax import lax
from jax.experimental import pallas as pl
from jax.experimental.pallas import tpu as pltpu
from jax.sharding import PartitionSpec as P

PHASE_RATE = 0.3
ALONG_SECOND = 1.7
DIRECTIONS = ((0.6, 0.48, 0.64), (-0.36, 0.8, 0.48))
F32 = jnp.float32
BF16 = jnp.bfloat16
CHUNKS = 2
AFTER = 2
LANES = 128


def partner_2(value, axis, bit):
    mask = 2**bit
    pairs = [(source, source ^ mask) for source in range(lax.axis_size(axis))]
    return lax.ppermute(value, axis, pairs)


def node_value(digits, order_count):
    return jnp.cos(math.pi * (2.0 * digits.astype(F32) + 1.0) / (2.0 * order_count))


def node_products(orders, operator_index, order_count):
    square = order_count * order_count
    direction = DIRECTIONS[operator_index]
    summed = direction[0] * node_value(orders // square, order_count)
    summed = summed + direction[1] * node_value(orders // order_count % order_count, order_count)
    return summed + direction[2] * node_value(orders % order_count, order_count)


def plan_levels(level_count, extents, locals_):
    levels = []
    for operator in range(2):
        top = extents[operator].bit_length() - 2
        local_bits = locals_[operator].bit_length() - 1
        for level in range(level_count):
            bit = top - level
            if bit >= local_bits:
                levels.append((operator, level, ("src", "tgt")[operator], bit - local_bits))
            else:
                levels.append((operator, level, None, bit))
    return levels


def cell(table, index):
    return table[index, 0], table[index, 1]


def prepare_body(levels, boxes_shape, first_other, orders_ref, turned_ref, reflection_ref, table_ref, spread_ref):
    boxes_u, boxes_v = boxes_shape
    boxes = boxes_u * boxes_v
    coef_count = orders_ref.shape[1]
    order_count = turned_ref.shape[2]
    orders = orders_ref[...]
    digits = (orders // (order_count * order_count), orders // order_count % order_count, orders % order_count)
    row = lax.broadcasted_iota(jnp.int32, (boxes, coef_count), 0)
    picked = jnp.where(row == 0, digits[0], jnp.where(row == 1, digits[1], digits[2]))
    values = node_value(picked, order_count)
    u = (row // boxes_v).astype(F32)
    v = (row % boxes_v).astype(F32)
    src = lax.axis_index("src")
    tgt = lax.axis_index("tgt")

    def corner(src_index):
        first = (src_index * boxes_u).astype(F32) + u + 0.5
        return first + ALONG_SECOND * ((tgt * boxes_v).astype(F32) + v + 0.5)

    def times(a, b):
        return a[0] * b[0] - a[1] * b[1], a[0] * b[1] + a[1] * b[0]

    def rounded(a):
        return a[0].astype(BF16).astype(F32), a[1].astype(BF16).astype(F32)

    def put(index, value):
        table_ref[index, 0] = value[0]
        table_ref[index, 1] = value[1]

    for operator in range(2):
        direction = DIRECTIONS[operator]
        products = direction[0] * values[0:1] + direction[1] * values[1:2] + direction[2] * values[2:3]
        angle = PHASE_RATE * corner(src) * products
        base = (jnp.cos(angle), jnp.sin(angle))
        power = base
        mine = [i for i, level in enumerate(levels) if level[0] == operator]
        for number, index in enumerate(mine):
            if number:
                power = times(power, base)
            phase = rounded(power)
            if operator == 1 and number == 0:
                weight = [
                    jnp.concatenate([reflection_ref[part, i] for i in range(boxes_u)], axis=0) for part in range(2)
                ]
                phase = times(phase, weight)
            put(index, phase)
        if operator == 0:
            angle = PHASE_RATE * corner(src ^ first_other) * products
            put(len(levels), rounded((jnp.cos(angle), jnp.sin(angle))))

    column = lax.broadcasted_iota(jnp.int32, (order_count, coef_count), 1)
    point = lax.broadcasted_iota(jnp.int32, (order_count, coef_count), 0)
    column_digits = (column // (order_count * order_count), column // order_count % order_count, column % order_count)
    for d in range(3):
        chosen = (column_digits[d] == point).astype(BF16)
        value = turned_ref[d]
        high = value.astype(BF16)
        rest = value - high.astype(F32)
        middle = rest.astype(BF16)
        low = (rest - middle.astype(F32)).astype(BF16)
        spread_ref[d] = dot(high, chosen) + (dot(middle, chosen) + dot(low, chosen))


def build_body(base, axis, bit, count, spread_ref, *w_refs):
    order_count = round(w_refs[0].shape[1] ** (1 / 3))
    square = order_count * order_count
    if axis is None:
        which = [base + i for i in range(count)]
    else:
        own = lax.axis_index(axis) >> bit & 1
        which = [base + 3 * own, base + own + 1]
    for number in range(count):
        begin = which[number] * order_count
        if axis is not None:
            begin = pl.multiple_of(begin, order_count)
        first, second, third = [spread_ref[d, pl.ds(begin, order_count)] for d in range(3)]
        w_ref = w_refs[number]
        for x in range(order_count):
            lead = first[x : x + 1] * second
            for y in range(0, order_count, 2):
                block = jnp.concatenate([lead[y : y + 1] * third, lead[y + 1 : y + 2] * third])
                w_ref[x * square + y * order_count : x * square + (y + 2) * order_count] = block.astype(BF16)


def modulate(src, table, index, dst, boxes, ill, place):
    half = boxes * ill
    for box in range(boxes):
        real = src[box * ill : (box + 1) * ill].astype(F32)
        imag = src[half + box * ill : half + (box + 1) * ill].astype(F32)
        cos = table[index, 0, box : box + 1]
        sin = table[index, 1, box : box + 1]
        dst[place(0, box)] = (cos * real - sin * imag).astype(BF16)
        dst[place(1, box)] = (cos * imag + sin * real).astype(BF16)


def strided(flat_ref, start, count, stride):
    return jnp.concatenate(
        [flat_ref[t, pl.ds(start, count, stride=stride)] for t in range(flat_ref.shape[0])], axis=1
    )


def modulate_raw(x_ref, table, index, flat_ref, dst):
    _, ill, boxes_u, boxes_v, _ = x_ref.shape
    boxes = boxes_u * boxes_v
    half = boxes * ill
    for part in range(2):
        for i in range(ill):
            for u in range(boxes_u):
                piece = x_ref[part, i, u].astype(F32)
                for t in range(flat_ref.shape[0]):
                    flat_ref[t, pl.ds(part * half + i * boxes + u * boxes_v, boxes_v)] = piece[:, t * LANES : (t + 1) * LANES]
    for box in range(boxes):
        real = strided(flat_ref, box, ill, boxes)
        imag = strided(flat_ref, half + box, ill, boxes)
        cos = table[index, 0, box : box + 1]
        sin = table[index, 1, box : box + 1]
        dst[box * ill : (box + 1) * ill] = (cos * real - sin * imag).astype(BF16)
        dst[half + box * ill : half + (box + 1) * ill] = (cos * imag + sin * real).astype(BF16)


def straight(boxes, ill):
    half = boxes * ill
    return lambda part, box: pl.ds(part * half + box * ill, ill)


def dot(a, b):
    return jnp.dot(a, b, preferred_element_type=F32)


def piece_body(begin, x_ref, *refs):
    out_ref, sem = refs[-2:]
    copy = pltpu.make_async_copy(x_ref.at[:, pl.ds(begin, out_ref.shape[1])], out_ref, sem)
    copy.start()
    copy.wait()


def own_body(index, raw, x_ref, table_ref, w_ref, out_ref, flat_ref, mod_ref):
    if raw:
        modulate_raw(x_ref, table_ref, index, flat_ref, mod_ref)
        out_ref[...] = dot(mod_ref[...], w_ref[...])
    else:
        out_ref[...] = dot(x_ref[...], w_ref[...])


def rest_body(shape, partner_index, pairs, send_index, begin, done, *refs):
    boxes_u, boxes_v, ill = shape
    boxes = boxes_u * boxes_v
    half = boxes * ill
    part_ref, got_ref, table_ref, w_ref = refs[:4]
    pair_refs = refs[4 : 4 + 4 * len(pairs)]
    if send_index is None:
        if done is None:
            turned_ref, state_ref, mod_ref, flat_ref = refs[-4:]
        else:
            out_ref, state_ref, mod_ref, flat_ref, turned_ref, sem = refs[-6:]
            copies = []
            for number in range(done):
                earlier = refs[4 + 4 * len(pairs) + number]
                place = pl.ds(number * ill, ill)
                copies.append(pltpu.make_async_copy(earlier, out_ref.at[:, place], sem.at[number]))
                copies[-1].start()
    else:
        out_ref, state_ref, mod_ref, flat_ref = refs[-4:]
    if partner_index is None:
        got = got_ref[...]
    else:
        modulate_raw(got_ref, table_ref, partner_index, flat_ref, mod_ref)
        got = mod_ref[...]
    state_ref[...] = part_ref[...] + dot(got, w_ref[...])
    for number, (index, operator, bit) in enumerate(pairs):
        w4 = pair_refs[4 * number : 4 * number + 4]
        box_bit = bit + (boxes_v.bit_length() - 1 if operator == 0 else 0)
        low_mask = (1 << box_bit) - 1

        def place(part, box):
            side = box >> box_bit & 1
            rank = (box >> (box_bit + 1) << box_bit) | (box & low_mask)
            return pl.ds(side * half + part * (half // 2) + rank * ill, ill)

        modulate(state_ref, table_ref, index, mod_ref, boxes, ill, place)
        for side in range(2):
            result = dot(mod_ref[:half], w4[2 * side][...]) + dot(mod_ref[half:], w4[2 * side + 1][...])
            for part in range(2):
                for box in range(boxes):
                    if box >> box_bit & 1 == side:
                        start = place(part, box).start - side * half
                        state_ref[straight(boxes, ill)(part, box)] = result[start : start + ill]
    if send_index is not None:
        modulate(state_ref, table_ref, send_index, out_ref, boxes, ill, straight(boxes, ill))
        return
    tiles = flat_ref.shape[0]
    for part in range(2):
        for box in range(boxes):
            value = state_ref[straight(boxes, ill)(part, box)]
            for t in range(tiles):
                flat_ref[t, pl.ds(part * half + box, ill, stride=boxes)] = value[:, t * LANES : (t + 1) * LANES]
    for part in range(2):
        for i in range(ill):
            for u in range(boxes_u):
                place = pl.ds(part * half + i * boxes + u * boxes_v, boxes_v)
                turned_ref[part, i, u] = jnp.concatenate([flat_ref[t, place] for t in range(tiles)], axis=1).astype(BF16)
    if done is not None:
        copies.append(pltpu.make_async_copy(turned_ref, out_ref.at[:, pl.ds(begin, ill)], sem.at[done]))
        copies[-1].start()
        for copy in copies:
            copy.wait()


def call(body, outs, scratch, flops, moved, name, *args, in_specs=None, out_specs=None, aliases=None, limit=6):
    vmem = pl.BlockSpec(memory_space=pltpu.VMEM)
    many = isinstance(outs, (tuple, list))
    return pl.pallas_call(
        body,
        out_shape=outs,
        in_specs=in_specs or [vmem] * len(args),
        out_specs=out_specs or ([vmem] * len(outs) if many else vmem),
        scratch_shapes=scratch,
        input_output_aliases=aliases or {},
        compiler_params=pltpu.CompilerParams(vmem_limit_bytes=limit * 1024 * 1024),
        cost_estimate=pl.CostEstimate(flops=flops, bytes_accessed=moved, transcendentals=0),
        name=name,
    )(*args)


def on_device(coeffs, reflection, interp, orders):
    level_count = interp.shape[1]
    order_count = interp.shape[-1]
    _, ill, boxes_u, boxes_v, coef_count = coeffs.shape
    boxes = boxes_u * boxes_v
    extents = (boxes_u * lax.axis_size("src"), boxes_v * lax.axis_size("tgt"))
    levels = plan_levels(level_count, extents, (boxes_u, boxes_v))
    assert levels[0][2] == "src"
    swaps = [i for i, level in enumerate(levels) if level[2] is not None]
    vmem = pl.BlockSpec(memory_space=pltpu.VMEM)
    anywhere = pl.BlockSpec(memory_space=pl.ANY)

    chunk = ill // CHUNKS if ill % CHUNKS == 0 else ill
    rows = 2 * boxes * chunk
    begins = list(range(0, ill, chunk))
    piece_shape = (2, chunk, boxes_u, boxes_v, coef_count)

    def piece(begin, after):
        return call(
            functools.partial(piece_body, begin),
            jax.ShapeDtypeStruct(piece_shape, BF16),
            [pltpu.SemaphoreType.DMA],
            1000,
            rows * coef_count * 4,
            f"piece_{begin}",
            coeffs,
            *after,
            in_specs=[anywhere] * (1 + len(after)),
        )

    pieces = [piece(begins[0], [])]

    turned = interp.reshape(-1, 3, order_count, order_count).transpose(1, 0, 3, 2).reshape(3, -1, order_count)
    table, spread = call(
        functools.partial(prepare_body, levels, (boxes_u, boxes_v), 2 ** levels[0][3]),
        [
            jax.ShapeDtypeStruct((len(levels) + 1, 2, boxes, coef_count), F32),
            jax.ShapeDtypeStruct((3, turned.shape[1], coef_count), F32),
        ],
        [],
        4000000,
        2000000,
        "prepare",
        orders.reshape(1, coef_count),
        turned,
        reflection,
    )
    matrices = []
    for index, (operator, level, axis, bit) in enumerate(levels):
        count = 4 if axis is None else 2
        matrices.append(
            call(
                functools.partial(build_body, (operator * level_count + level) * 4, axis, bit, count),
                [jax.ShapeDtypeStruct((coef_count, coef_count), BF16)] * count,
                [],
                count * 20000000,
                count * 2 * coef_count * coef_count,
                f"build_{index}",
                spread,
            )
        )

    for number, begin in enumerate(begins[1:]):
        pieces.append(piece(begin, [matrices[AFTER][1]]))
    raws = [partner_2(value, levels[0][2], levels[0][3]) for value in pieces]

    product_flops = 2 * rows * coef_count * coef_count

    def own_part(number, current):
        index = swaps[number]
        return call(
            functools.partial(own_body, index, number == 0),
            jax.ShapeDtypeStruct((rows, coef_count), F32),
            [pltpu.VMEM((coef_count // LANES, rows, LANES), F32), pltpu.VMEM((rows, coef_count), BF16)],
            product_flops,
            rows * coef_count * 6 + coef_count * coef_count * 2,
            f"own_{index}",
            current,
            table,
            matrices[index][0],
        )

    def rest_part(number, own, partner, begin, earlier):
        index = swaps[number]
        last = number + 1 == len(swaps)
        after = len(levels) if last else swaps[number + 1]
        pairs = [(i, levels[i][0], levels[i][3]) for i in range(index + 1, after)]
        args = [own, partner, table, matrices[index][1]]
        for i, _, _ in pairs:
            args += matrices[i]
        specs = [vmem] * len(args)
        scratch = [
            pltpu.VMEM((rows, coef_count), F32),
            pltpu.VMEM((rows, coef_count), BF16),
            pltpu.VMEM((coef_count // LANES, rows, LANES), F32),
        ]
        out = jax.ShapeDtypeStruct((rows, coef_count), BF16)
        out_specs, done = vmem, None
        if last and begin < begins[-1]:
            out = jax.ShapeDtypeStruct(piece_shape, BF16)
        elif last:
            out = jax.ShapeDtypeStruct(coeffs.shape, BF16)
            out_specs, done = anywhere, len(earlier)
            scratch += [pltpu.VMEM(piece_shape, BF16), pltpu.SemaphoreType.DMA((len(begins),))]
            args += earlier
            specs += [vmem] * len(earlier)
        return call(
            functools.partial(
                rest_body,
                (boxes_u, boxes_v, chunk),
                len(levels) if number == 0 else None,
                pairs,
                None if last else after,
                begin,
                done,
            ),
            out,
            scratch,
            product_flops * (1 + 2 * len(pairs)),
            rows * coef_count * 8 + coef_count * coef_count * 2 * (1 + 4 * len(pairs)),
            f"rest_{index}",
            *args,
            in_specs=specs,
            out_specs=out_specs,
        )

    currents, gots = pieces, raws
    for number, index in enumerate(swaps):
        if number:
            gots = [partner_2(current, levels[index][2], levels[index][3]) for current in currents]
        owns = [own_part(number, current) for current in currents]
        following = []
        for own, got, begin in zip(owns, gots, begins):
            following.append(rest_part(number, own, got, begin, following))
        currents = following
    return currents[-1]


def solution(mesh):
    in_specs = (
        P(None, ("groups", "ill"), "src", "tgt", None),
        P(None, ("groups", "src"), "tgt", None),
        P(),
        P(),
    )
    out_specs = P(None, ("groups", "ill"), "src", "tgt", None)
    return jax.shard_map(
        on_device, mesh=mesh, in_specs=in_specs, out_specs=out_specs, check_vma=False
    )
```

```python
import functools
import math

import jax
import jax.numpy as jnp
from jax import lax
from jax.experimental import pallas as pl
from jax.experimental.pallas import tpu as pltpu
from jax.sharding import PartitionSpec as P


PHASE_RATE = 0.3
ALONG_SECOND = 1.7
DIRECTIONS = ((0.6, 0.48, 0.64), (-0.36, 0.8, 0.48))
F32 = jnp.float32
BF16 = jnp.bfloat16
CHUNKS = 2
LANES = 128
EARLY = 4


def partner_2(value, axis, bit):
    mask = 2**bit
    pairs = [(source, source ^ mask) for source in range(lax.axis_size(axis))]
    return lax.ppermute(value, axis, pairs)


def node_value(digits, order_count):
    return jnp.cos(math.pi * (2.0 * digits.astype(F32) + 1.0) / (2.0 * order_count))


def plan_levels(level_count, extents, locals_):
    levels = []
    for operator in range(2):
        top = extents[operator].bit_length() - 2
        local_bits = locals_[operator].bit_length() - 1
        for level in range(level_count):
            bit = top - level
            if bit >= local_bits:
                levels.append((operator, level, ("src", "tgt")[operator], bit - local_bits))
            else:
                levels.append((operator, level, None, bit))
    return levels


def table_body(levels, boxes_shape, first_other, order_count, orders_ref, reflection_ref, table_ref):
    boxes_u, boxes_v = boxes_shape
    boxes = boxes_u * boxes_v
    coef_count = orders_ref.shape[1]
    orders = orders_ref[...]
    digits = (orders // (order_count * order_count), orders // order_count % order_count, orders % order_count)
    row = lax.broadcasted_iota(jnp.int32, (boxes, coef_count), 0)
    picked = jnp.where(row == 0, digits[0], jnp.where(row == 1, digits[1], digits[2]))
    values = node_value(picked, order_count)
    u = (row // boxes_v).astype(F32)
    v = (row % boxes_v).astype(F32)
    src = lax.axis_index("src")
    tgt = lax.axis_index("tgt")

    def corner(src_index):
        first = (src_index * boxes_u).astype(F32) + u + 0.5
        return first + ALONG_SECOND * ((tgt * boxes_v).astype(F32) + v + 0.5)

    def times(a, b):
        return a[0] * b[0] - a[1] * b[1], a[0] * b[1] + a[1] * b[0]

    def rounded(a):
        return a[0].astype(BF16).astype(F32), a[1].astype(BF16).astype(F32)

    def put(index, value):
        table_ref[index, 0] = value[0]
        table_ref[index, 1] = value[1]

    for operator in range(2):
        direction = DIRECTIONS[operator]
        products = direction[0] * values[0:1] + direction[1] * values[1:2] + direction[2] * values[2:3]
        angle = PHASE_RATE * corner(src) * products
        base = (jnp.cos(angle), jnp.sin(angle))
        power = base
        mine = [i for i, level in enumerate(levels) if level[0] == operator]
        for number, index in enumerate(mine):
            if number:
                power = times(power, base)
            phase = rounded(power)
            if operator == 1 and number == 0:
                weight = [
                    jnp.concatenate([reflection_ref[part, i] for i in range(boxes_u)], axis=0) for part in range(2)
                ]
                phase = times(phase, weight)
            put(index, phase)
        if operator == 0:
            angle = PHASE_RATE * corner(src ^ first_other) * products
            put(len(levels), rounded((jnp.cos(angle), jnp.sin(angle))))


def spread_body(interp_ref, spread_ref):
    order_count = interp_ref.shape[-1]
    coef_count = spread_ref.shape[-1]
    column = lax.broadcasted_iota(jnp.int32, (order_count, coef_count), 1)
    point = lax.broadcasted_iota(jnp.int32, (order_count, coef_count), 0)
    column_digits = (column // (order_count * order_count), column // order_count % order_count, column % order_count)
    for d in range(3):
        chosen = (column_digits[d] == point).astype(BF16)
        value = jnp.swapaxes(interp_ref[:, d], 1, 2).reshape(-1, order_count)
        high = value.astype(BF16)
        rest = value - high.astype(F32)
        middle = rest.astype(BF16)
        low = (rest - middle.astype(F32)).astype(BF16)
        spread_ref[d] = dot(high, chosen) + (dot(middle, chosen) + dot(low, chosen))


def build_body(base, axis, bit, count, spread_ref, *w_refs):
    order_count = round(w_refs[0].shape[1] ** (1 / 3))
    square = order_count * order_count
    if axis is None:
        which = [base + i for i in range(count)]
    else:
        own = lax.axis_index(axis) >> bit & 1
        which = [base + 3 * own, base + own + 1]
    for number in range(count):
        begin = which[number] * order_count
        if axis is not None:
            begin = pl.multiple_of(begin, order_count)
        first, second, third = [spread_ref[d, pl.ds(begin, order_count)] for d in range(3)]
        w_ref = w_refs[number]
        for x in range(order_count):
            lead = first[x : x + 1] * second
            for y in range(0, order_count, 2):
                block = jnp.concatenate([lead[y : y + 1] * third, lead[y + 1 : y + 2] * third])
                w_ref[x * square + y * order_count : x * square + (y + 2) * order_count] = block.astype(BF16)


def modulate(src, table, index, dst, boxes, ill, place):
    half = boxes * ill
    for box in range(boxes):
        real = src[box * ill : (box + 1) * ill].astype(F32)
        imag = src[half + box * ill : half + (box + 1) * ill].astype(F32)
        cos = table[index, 0, box : box + 1]
        sin = table[index, 1, box : box + 1]
        dst[place(0, box)] = (cos * real - sin * imag).astype(BF16)
        dst[place(1, box)] = (cos * imag + sin * real).astype(BF16)


def strided(flat_ref, start, count, stride):
    return jnp.concatenate(
        [flat_ref[t, pl.ds(start, count, stride=stride)] for t in range(flat_ref.shape[0])], axis=1
    )


def modulate_raw(x_ref, table, index, flat_ref, dst):
    _, ill, boxes_u, boxes_v, _ = x_ref.shape
    boxes = boxes_u * boxes_v
    half = boxes * ill
    for part in range(2):
        for i in range(ill):
            for u in range(boxes_u):
                piece = x_ref[part, i, u].astype(F32)
                for t in range(flat_ref.shape[0]):
                    flat_ref[t, pl.ds(part * half + i * boxes + u * boxes_v, boxes_v)] = piece[:, t * LANES : (t + 1) * LANES]
    for box in range(boxes):
        real = strided(flat_ref, box, ill, boxes)
        imag = strided(flat_ref, half + box, ill, boxes)
        cos = table[index, 0, box : box + 1]
        sin = table[index, 1, box : box + 1]
        dst[box * ill : (box + 1) * ill] = (cos * real - sin * imag).astype(BF16)
        dst[half + box * ill : half + (box + 1) * ill] = (cos * imag + sin * real).astype(BF16)


def straight(boxes, ill):
    half = boxes * ill
    return lambda part, box: pl.ds(part * half + box * ill, ill)


def dot(a, b):
    return jnp.dot(a, b, preferred_element_type=F32)


def piece_body(begin, x_ref, *refs):
    out_ref, sem = refs[-2:]
    copy = pltpu.make_async_copy(x_ref.at[:, pl.ds(begin, out_ref.shape[1])], out_ref, sem)
    copy.start()
    copy.wait()


def own_body(index, raw, x_ref, table_ref, w_ref, out_ref, flat_ref, mod_ref):
    if raw:
        modulate_raw(x_ref, table_ref, index, flat_ref, mod_ref)
        out_ref[...] = dot(mod_ref[...], w_ref[...])
    else:
        out_ref[...] = dot(x_ref[...], w_ref[...])


def rest_body(shape, partner_index, pairs, send_index, begin, done, *refs):
    boxes_u, boxes_v, ill = shape
    boxes = boxes_u * boxes_v
    half = boxes * ill
    part_ref, got_ref, table_ref, w_ref = refs[:4]
    pair_refs = refs[4 : 4 + 4 * len(pairs)]
    if send_index is None:
        if done is None:
            turned_ref, state_ref, mod_ref, flat_ref = refs[-4:]
        else:
            out_ref, state_ref, mod_ref, flat_ref, turned_ref, sem = refs[-6:]
            copies = []
            for number in range(done):
                earlier = refs[4 + 4 * len(pairs) + number]
                place = pl.ds(number * ill, ill)
                copies.append(pltpu.make_async_copy(earlier, out_ref.at[:, place], sem.at[number]))
                copies[-1].start()
    else:
        out_ref, state_ref, mod_ref, flat_ref = refs[-4:]
    if partner_index is None:
        got = got_ref[...]
    else:
        modulate_raw(got_ref, table_ref, partner_index, flat_ref, mod_ref)
        got = mod_ref[...]
    state_ref[...] = part_ref[...] + dot(got, w_ref[...])
    for number, (index, operator, bit) in enumerate(pairs):
        w4 = pair_refs[4 * number : 4 * number + 4]
        box_bit = bit + (boxes_v.bit_length() - 1 if operator == 0 else 0)
        low_mask = (1 << box_bit) - 1

        def place(part, box):
            side = box >> box_bit & 1
            rank = (box >> (box_bit + 1) << box_bit) | (box & low_mask)
            return pl.ds(side * half + part * (half // 2) + rank * ill, ill)

        modulate(state_ref, table_ref, index, mod_ref, boxes, ill, place)
        for side in range(2):
            result = dot(mod_ref[:half], w4[2 * side][...]) + dot(mod_ref[half:], w4[2 * side + 1][...])
            for part in range(2):
                for box in range(boxes):
                    if box >> box_bit & 1 == side:
                        start = place(part, box).start - side * half
                        state_ref[straight(boxes, ill)(part, box)] = result[start : start + ill]
    if send_index is not None:
        modulate(state_ref, table_ref, send_index, out_ref, boxes, ill, straight(boxes, ill))
        return
    tiles = flat_ref.shape[0]
    for part in range(2):
        for box in range(boxes):
            value = state_ref[straight(boxes, ill)(part, box)]
            for t in range(tiles):
                flat_ref[t, pl.ds(part * half + box, ill, stride=boxes)] = value[:, t * LANES : (t + 1) * LANES]
        for i in range(ill):
            for u in range(boxes_u):
                place = pl.ds(part * half + i * boxes + u * boxes_v, boxes_v)
                turned_ref[part, i, u] = jnp.concatenate([flat_ref[t, place] for t in range(tiles)], axis=1).astype(BF16)
        if done is not None:
            target = out_ref.at[part, pl.ds(begin, ill)]
            copies.append(pltpu.make_async_copy(turned_ref.at[part], target, sem.at[done + part]))
            copies[-1].start()
    if done is not None:
        for copy in copies:
            copy.wait()


def call(body, outs, scratch, flops, moved, *args, in_specs=None, out_specs=None, aliases=None, limit=6 * 1024 * 1024):
    vmem = pl.BlockSpec(memory_space=pltpu.VMEM)
    many = isinstance(outs, (tuple, list))
    return pl.pallas_call(
        body,
        out_shape=outs,
        in_specs=in_specs or [vmem] * len(args),
        out_specs=out_specs or ([vmem] * len(outs) if many else vmem),
        scratch_shapes=scratch,
        input_output_aliases=aliases or {},
        compiler_params=pltpu.CompilerParams(vmem_limit_bytes=limit),
        cost_estimate=pl.CostEstimate(flops=flops, bytes_accessed=moved, transcendentals=0),
    )(*args)


def on_device(coeffs, reflection, interp, orders):
    level_count = interp.shape[1]
    order_count = interp.shape[-1]
    _, ill, boxes_u, boxes_v, coef_count = coeffs.shape
    boxes = boxes_u * boxes_v
    extents = (boxes_u * lax.axis_size("src"), boxes_v * lax.axis_size("tgt"))
    levels = plan_levels(level_count, extents, (boxes_u, boxes_v))
    assert levels[0][2] == "src"
    swaps = [i for i, level in enumerate(levels) if level[2] is not None]
    vmem = pl.BlockSpec(memory_space=pltpu.VMEM)
    anywhere = pl.BlockSpec(memory_space=pl.ANY)

    chunk = ill // CHUNKS if ill % CHUNKS == 0 else ill
    rows = 2 * boxes * chunk
    begins = list(range(0, ill, chunk))
    piece_shape = (2, chunk, boxes_u, boxes_v, coef_count)

    def piece(begin, after):
        return call(
            functools.partial(piece_body, begin),
            jax.ShapeDtypeStruct(piece_shape, BF16),
            [pltpu.SemaphoreType.DMA],
            1000,
            rows * coef_count * 4,
            coeffs,
            *after,
            in_specs=[anywhere] * (1 + len(after)),
            limit=6 * 1024 * 1024,
        )

    pieces = [coeffs[:, :chunk]]

    factors = interp.reshape(-1, 3, order_count, order_count)
    spread = call(
        spread_body,
        jax.ShapeDtypeStruct((3, factors.shape[0] * order_count, coef_count), F32),
        [],
        2000000,
        1000000,
        factors,
    )
    table = call(
        functools.partial(table_body, levels, (boxes_u, boxes_v), 2 ** levels[0][3], order_count),
        jax.ShapeDtypeStruct((len(levels) + 1, 2, boxes, coef_count), F32),
        [],
        2000000,
        1000000,
        orders.reshape(1, coef_count),
        reflection,
    )
    matrices = []
    for operator, level, axis, bit in levels:
        count = 4 if axis is None else 2
        matrices.append(
            call(
                functools.partial(build_body, (operator * level_count + level) * 4, axis, bit, count),
                [jax.ShapeDtypeStruct((coef_count, coef_count), BF16)] * count,
                [],
                count * 20000000,
                count * 2 * coef_count * coef_count,
                spread,
            )
        )

    for begin in begins[1:]:
        pieces.append(piece(begin, [table] + [w[1] for w in matrices[:EARLY]]))
    raws = []
    for value in pieces:
        raws.append(partner_2(value, levels[0][2], levels[0][3]))

    product_flops = 2 * rows * coef_count * coef_count

    def own_part(number, current):
        index = swaps[number]
        return call(
            functools.partial(own_body, index, number == 0),
            jax.ShapeDtypeStruct((rows, coef_count), F32),
            [pltpu.VMEM((coef_count // LANES, rows, LANES), F32), pltpu.VMEM((rows, coef_count), BF16)],
            product_flops,
            rows * coef_count * 6 + coef_count * coef_count * 2,
            current,
            table,
            matrices[index][0],
        )

    def rest_part(number, own, partner, begin, earlier):
        index = swaps[number]
        last = number + 1 == len(swaps)
        after = len(levels) if last else swaps[number + 1]
        pairs = [(i, levels[i][0], levels[i][3]) for i in range(index + 1, after)]
        args = [own, partner, table, matrices[index][1]]
        for i, _, _ in pairs:
            args += matrices[i]
        specs = [vmem] * len(args)
        scratch = [
            pltpu.VMEM((rows, coef_count), F32),
            pltpu.VMEM((rows, coef_count), BF16),
            pltpu.VMEM((coef_count // LANES, rows, LANES), F32),
        ]
        out = jax.ShapeDtypeStruct((rows, coef_count), BF16)
        out_specs, done = vmem, None
        if last and begin < begins[-1]:
            out = jax.ShapeDtypeStruct(piece_shape, BF16)
        elif last:
            out = jax.ShapeDtypeStruct(coeffs.shape, BF16)
            out_specs, done = anywhere, len(earlier)
            scratch += [pltpu.VMEM(piece_shape, BF16), pltpu.SemaphoreType.DMA((len(begins) + 1,))]
            args += earlier
            specs += [vmem] * len(earlier)
        return call(
            functools.partial(
                rest_body,
                (boxes_u, boxes_v, chunk),
                len(levels) if number == 0 else None,
                pairs,
                None if last else after,
                begin,
                done,
            ),
            out,
            scratch,
            product_flops * (1 + 2 * len(pairs)),
            rows * coef_count * 8 + coef_count * coef_count * 2 * (1 + 4 * len(pairs)),
            *args,
            in_specs=specs,
            out_specs=out_specs,
        )

    currents, gots = pieces, raws
    for number, index in enumerate(swaps):
        if number:
            gots = []
            for current in currents:
                gots.append(partner_2(current, levels[index][2], levels[index][3]))
        owns = [own_part(number, current) for current in currents]
        following = []
        for own, got, begin in zip(owns, gots, begins):
            following.append(rest_part(number, own, got, begin, following))
        currents = following
    return currents[-1]


def solution(mesh):
    in_specs = (
        P(None, ("groups", "ill"), "src", "tgt", None),
        P(None, ("groups", "src"), "tgt", None),
        P(),
        P(),
    )
    out_specs = P(None, ("groups", "ill"), "src", "tgt", None)

    return jax.shard_map(on_device, mesh=mesh, in_specs=in_specs, out_specs=out_specs, check_vma=False)
```

```python
import functools
import math

import jax
import jax.numpy as jnp
from jax import lax
from jax.experimental import pallas as pl
from jax.experimental.pallas import tpu as pltpu
from jax.sharding import PartitionSpec as P


PHASE_RATE = 0.3
ALONG_SECOND = 1.7
DIRECTIONS = ((0.6, 0.48, 0.64), (-0.36, 0.8, 0.48))
F32 = jnp.float32
BF16 = jnp.bfloat16
CHUNKS = 2
LANES = 128
EARLY = 2


def partner_2(value, axis, bit):
    mask = 2**bit
    pairs = [(source, source ^ mask) for source in range(lax.axis_size(axis))]
    return lax.ppermute(value, axis, pairs)


def node_value(digits, order_count):
    return jnp.cos(math.pi * (2.0 * digits.astype(F32) + 1.0) / (2.0 * order_count))


def plan_levels(level_count, extents, locals_):
    levels = []
    for operator in range(2):
        top = extents[operator].bit_length() - 2
        local_bits = locals_[operator].bit_length() - 1
        for level in range(level_count):
            bit = top - level
            if bit >= local_bits:
                levels.append((operator, level, ("src", "tgt")[operator], bit - local_bits))
            else:
                levels.append((operator, level, None, bit))
    return levels


def table_body(levels, boxes_shape, first_other, order_count, orders_ref, reflection_ref, table_ref):
    boxes_u, boxes_v = boxes_shape
    boxes = boxes_u * boxes_v
    coef_count = orders_ref.shape[1]
    orders = orders_ref[...]
    digits = (orders // (order_count * order_count), orders // order_count % order_count, orders % order_count)
    row = lax.broadcasted_iota(jnp.int32, (boxes, coef_count), 0)
    picked = jnp.where(row == 0, digits[0], jnp.where(row == 1, digits[1], digits[2]))
    values = node_value(picked, order_count)
    u = (row // boxes_v).astype(F32)
    v = (row % boxes_v).astype(F32)
    src = lax.axis_index("src")
    tgt = lax.axis_index("tgt")

    def corner(src_index):
        first = (src_index * boxes_u).astype(F32) + u + 0.5
        return first + ALONG_SECOND * ((tgt * boxes_v).astype(F32) + v + 0.5)

    def times(a, b):
        return a[0] * b[0] - a[1] * b[1], a[0] * b[1] + a[1] * b[0]

    def rounded(a):
        return a[0].astype(BF16).astype(F32), a[1].astype(BF16).astype(F32)

    def put(index, value):
        table_ref[index, 0] = value[0]
        table_ref[index, 1] = value[1]

    for operator in range(2):
        direction = DIRECTIONS[operator]
        products = direction[0] * values[0:1] + direction[1] * values[1:2] + direction[2] * values[2:3]
        angle = PHASE_RATE * corner(src) * products
        base = (jnp.cos(angle), jnp.sin(angle))
        power = base
        mine = [i for i, level in enumerate(levels) if level[0] == operator]
        for number, index in enumerate(mine):
            if number:
                power = times(power, base)
            phase = rounded(power)
            if operator == 1 and number == 0:
                weight = [
                    jnp.concatenate([reflection_ref[part, i] for i in range(boxes_u)], axis=0) for part in range(2)
                ]
                phase = times(phase, weight)
            put(index, phase)
        if operator == 0:
            angle = PHASE_RATE * corner(src ^ first_other) * products
            put(len(levels), rounded((jnp.cos(angle), jnp.sin(angle))))


def spread_body(interp_ref, spread_ref):
    order_count = interp_ref.shape[-1]
    coef_count = spread_ref.shape[-1]
    column = lax.broadcasted_iota(jnp.int32, (order_count, coef_count), 1)
    point = lax.broadcasted_iota(jnp.int32, (order_count, coef_count), 0)
    column_digits = (column // (order_count * order_count), column // order_count % order_count, column % order_count)
    for d in range(3):
        chosen = (column_digits[d] == point).astype(BF16)
        value = jnp.swapaxes(interp_ref[:, d], 1, 2).reshape(-1, order_count)
        high = value.astype(BF16)
        rest = value - high.astype(F32)
        middle = rest.astype(BF16)
        low = (rest - middle.astype(F32)).astype(BF16)
        spread_ref[d] = dot(high, chosen) + (dot(middle, chosen) + dot(low, chosen))


def build_body(base, axis, bit, count, spread_ref, *w_refs):
    order_count = round(w_refs[0].shape[1] ** (1 / 3))
    square = order_count * order_count
    if axis is None:
        which = [base + i for i in range(count)]
    else:
        own = lax.axis_index(axis) >> bit & 1
        which = [base + 3 * own, base + own + 1]
    for number in range(count):
        begin = which[number] * order_count
        if axis is not None:
            begin = pl.multiple_of(begin, order_count)
        first, second, third = [spread_ref[d, pl.ds(begin, order_count)] for d in range(3)]
        w_ref = w_refs[number]
        for x in range(order_count):
            lead = first[x : x + 1] * second
            for y in range(0, order_count, 2):
                block = jnp.concatenate([lead[y : y + 1] * third, lead[y + 1 : y + 2] * third])
                w_ref[x * square + y * order_count : x * square + (y + 2) * order_count] = block.astype(BF16)


def modulate(src, table, index, dst, boxes, ill, place):
    half = boxes * ill
    for box in range(boxes):
        real = src[box * ill : (box + 1) * ill].astype(F32)
        imag = src[half + box * ill : half + (box + 1) * ill].astype(F32)
        cos = table[index, 0, box : box + 1]
        sin = table[index, 1, box : box + 1]
        dst[place(0, box)] = (cos * real - sin * imag).astype(BF16)
        dst[place(1, box)] = (cos * imag + sin * real).astype(BF16)


def strided(flat_ref, start, count, stride):
    return jnp.concatenate(
        [flat_ref[t, pl.ds(start, count, stride=stride)] for t in range(flat_ref.shape[0])], axis=1
    )


def modulate_raw(x_ref, table, index, flat_ref, dst):
    _, ill, boxes_u, boxes_v, _ = x_ref.shape
    boxes = boxes_u * boxes_v
    half = boxes * ill
    for part in range(2):
        for i in range(ill):
            for u in range(boxes_u):
                piece = x_ref[part, i, u].astype(F32)
                for t in range(flat_ref.shape[0]):
                    flat_ref[t, pl.ds(part * half + i * boxes + u * boxes_v, boxes_v)] = piece[:, t * LANES : (t + 1) * LANES]
    for box in range(boxes):
        real = strided(flat_ref, box, ill, boxes)
        imag = strided(flat_ref, half + box, ill, boxes)
        cos = table[index, 0, box : box + 1]
        sin = table[index, 1, box : box + 1]
        dst[box * ill : (box + 1) * ill] = (cos * real - sin * imag).astype(BF16)
        dst[half + box * ill : half + (box + 1) * ill] = (cos * imag + sin * real).astype(BF16)


def straight(boxes, ill):
    half = boxes * ill
    return lambda part, box: pl.ds(part * half + box * ill, ill)


def dot(a, b):
    return jnp.dot(a, b, preferred_element_type=F32)


def piece_body(begin, x_ref, *refs):
    out_ref, flat_ref = refs[-2:]
    _, _, boxes_u, boxes_v, _ = x_ref.shape
    boxes = boxes_u * boxes_v
    ill = out_ref.shape[0] // (2 * boxes)
    half = boxes * ill
    for part in range(2):
        for i in range(ill):
            for u in range(boxes_u):
                piece = x_ref[part, begin + i, u].astype(F32)
                place = pl.ds(part * half + i * boxes + u * boxes_v, boxes_v)
                for t in range(flat_ref.shape[0]):
                    flat_ref[t, place] = piece[:, t * LANES : (t + 1) * LANES]
        for box in range(boxes):
            value = strided(flat_ref, part * half + box, ill, boxes)
            out_ref[part * half + box * ill : part * half + (box + 1) * ill] = value.astype(BF16)


def own_body(index, x_ref, table_ref, w_ref, out_ref, flat_ref, mod_ref):
    if index is None:
        out_ref[...] = dot(x_ref[...], w_ref[...])
    else:
        receive(x_ref, table_ref, index, flat_ref, mod_ref)
        out_ref[...] = dot(mod_ref[...], w_ref[...])


def receive(x_ref, table_ref, index, flat_ref, mod_ref):
    if len(x_ref.shape) == 5:
        modulate_raw(x_ref, table_ref, index, flat_ref, mod_ref)
    else:
        boxes = table_ref.shape[2]
        ill = x_ref.shape[0] // (2 * boxes)
        modulate(x_ref, table_ref, index, mod_ref, boxes, ill, straight(boxes, ill))


def rest_body(shape, partner_index, pairs, send_index, begin, done, *refs):
    boxes_u, boxes_v, ill = shape
    boxes = boxes_u * boxes_v
    half = boxes * ill
    part_ref, got_ref, table_ref, w_ref = refs[:4]
    pair_refs = refs[4 : 4 + 4 * len(pairs)]
    if send_index is None:
        if done is None:
            turned_ref, state_ref, mod_ref, flat_ref = refs[-4:]
        else:
            out_ref, state_ref, mod_ref, flat_ref, turned_ref, sem = refs[-6:]
            copies = []
            for number in range(done):
                earlier = refs[4 + 4 * len(pairs) + number]
                place = pl.ds(number * ill, ill)
                copies.append(pltpu.make_async_copy(earlier, out_ref.at[:, place], sem.at[number]))
                copies[-1].start()
    else:
        out_ref, state_ref, mod_ref, flat_ref = refs[-4:]
    if partner_index is None:
        got = got_ref[...]
    else:
        receive(got_ref, table_ref, partner_index, flat_ref, mod_ref)
        got = mod_ref[...]
    state_ref[...] = part_ref[...] + dot(got, w_ref[...])
    for number, (index, operator, bit) in enumerate(pairs):
        w4 = pair_refs[4 * number : 4 * number + 4]
        box_bit = bit + (boxes_v.bit_length() - 1 if operator == 0 else 0)
        low_mask = (1 << box_bit) - 1

        def place(part, box):
            side = box >> box_bit & 1
            rank = (box >> (box_bit + 1) << box_bit) | (box & low_mask)
            return pl.ds(side * half + part * (half // 2) + rank * ill, ill)

        modulate(state_ref, table_ref, index, mod_ref, boxes, ill, place)
        for side in range(2):
            result = dot(mod_ref[:half], w4[2 * side][...]) + dot(mod_ref[half:], w4[2 * side + 1][...])
            for part in range(2):
                for box in range(boxes):
                    if box >> box_bit & 1 == side:
                        start = place(part, box).start - side * half
                        value = result[start : start + ill]
                        if send_index is None and number + 1 == len(pairs):
                            for t in range(flat_ref.shape[0]):
                                lanes = slice(t * LANES, (t + 1) * LANES)
                                flat_ref[t, pl.ds(part * half + box, ill, stride=boxes)] = value[:, lanes]
                        else:
                            state_ref[straight(boxes, ill)(part, box)] = value
    if send_index is not None:
        modulate(state_ref, table_ref, send_index, out_ref, boxes, ill, straight(boxes, ill))
        return
    tiles = flat_ref.shape[0]
    for part in range(2):
        for box in range(0 if pairs else boxes):
            value = state_ref[straight(boxes, ill)(part, box)]
            for t in range(tiles):
                flat_ref[t, pl.ds(part * half + box, ill, stride=boxes)] = value[:, t * LANES : (t + 1) * LANES]
        for i in range(ill):
            for u in range(boxes_u):
                place = pl.ds(part * half + i * boxes + u * boxes_v, boxes_v)
                turned_ref[part, i, u] = jnp.concatenate([flat_ref[t, place] for t in range(tiles)], axis=1).astype(BF16)
        if done is not None:
            target = out_ref.at[part, pl.ds(begin, ill)]
            copies.append(pltpu.make_async_copy(turned_ref.at[part], target, sem.at[done + part]))
            copies[-1].start()
    if done is not None:
        for copy in copies:
            copy.wait()


def call(body, outs, scratch, flops, moved, *args, in_specs=None, out_specs=None, aliases=None, limit=6 * 1024 * 1024):
    vmem = pl.BlockSpec(memory_space=pltpu.VMEM)
    many = isinstance(outs, (tuple, list))
    return pl.pallas_call(
        body,
        out_shape=outs,
        in_specs=in_specs or [vmem] * len(args),
        out_specs=out_specs or ([vmem] * len(outs) if many else vmem),
        scratch_shapes=scratch,
        input_output_aliases=aliases or {},
        compiler_params=pltpu.CompilerParams(vmem_limit_bytes=limit),
        cost_estimate=pl.CostEstimate(flops=flops, bytes_accessed=moved, transcendentals=0),
    )(*args)


def on_device(coeffs, reflection, interp, orders):
    level_count = interp.shape[1]
    order_count = interp.shape[-1]
    _, ill, boxes_u, boxes_v, coef_count = coeffs.shape
    boxes = boxes_u * boxes_v
    extents = (boxes_u * lax.axis_size("src"), boxes_v * lax.axis_size("tgt"))
    levels = plan_levels(level_count, extents, (boxes_u, boxes_v))
    assert levels[0][2] == "src"
    swaps = [i for i, level in enumerate(levels) if level[2] is not None]
    vmem = pl.BlockSpec(memory_space=pltpu.VMEM)
    anywhere = pl.BlockSpec(memory_space=pl.ANY)

    chunk = ill // CHUNKS if ill % CHUNKS == 0 else ill
    rows = 2 * boxes * chunk
    begins = list(range(0, ill, chunk))
    piece_shape = (2, chunk, boxes_u, boxes_v, coef_count)

    def piece(begin, after):
        return call(
            functools.partial(piece_body, begin),
            jax.ShapeDtypeStruct((rows, coef_count), BF16),
            [pltpu.VMEM((coef_count // LANES, rows, LANES), F32)],
            1000,
            rows * coef_count * 4,
            coeffs,
            *after,
            in_specs=[vmem] + [anywhere] * len(after),
        )

    pieces = [coeffs[:, :chunk]]

    factors = interp.reshape(-1, 3, order_count, order_count)
    spread = call(
        spread_body,
        jax.ShapeDtypeStruct((3, factors.shape[0] * order_count, coef_count), F32),
        [],
        2000000,
        1000000,
        factors,
    )
    table = call(
        functools.partial(table_body, levels, (boxes_u, boxes_v), 2 ** levels[0][3], order_count),
        jax.ShapeDtypeStruct((len(levels) + 1, 2, boxes, coef_count), F32),
        [],
        2000000,
        1000000,
        orders.reshape(1, coef_count),
        reflection,
    )
    matrices = []
    for operator, level, axis, bit in levels:
        count = 4 if axis is None else 2
        matrices.append(
            call(
                functools.partial(build_body, (operator * level_count + level) * 4, axis, bit, count),
                [jax.ShapeDtypeStruct((coef_count, coef_count), BF16)] * count,
                [],
                count * 20000000,
                count * 2 * coef_count * coef_count,
                spread,
            )
        )

    for begin in begins[1:]:
        pieces.append(piece(begin, [table] + [w[1] for w in matrices[:EARLY]]))
    raws = []
    for value in pieces:
        raws.append(partner_2(value, levels[0][2], levels[0][3]))

    product_flops = 2 * rows * coef_count * coef_count

    def own_part(number, current):
        index = swaps[number]
        return call(
            functools.partial(own_body, index if number == 0 else None),
            jax.ShapeDtypeStruct((rows, coef_count), F32),
            [pltpu.VMEM((coef_count // LANES, rows, LANES), F32), pltpu.VMEM((rows, coef_count), BF16)],
            product_flops,
            rows * coef_count * 6 + coef_count * coef_count * 2,
            current,
            table,
            matrices[index][0],
        )

    def rest_part(number, own, partner, begin, earlier):
        index = swaps[number]
        last = number + 1 == len(swaps)
        after = len(levels) if last else swaps[number + 1]
        pairs = [(i, levels[i][0], levels[i][3]) for i in range(index + 1, after)]
        args = [own, partner, table, matrices[index][1]]
        for i, _, _ in pairs:
            args += matrices[i]
        specs = [vmem] * len(args)
        scratch = [
            pltpu.VMEM((rows, coef_count), F32),
            pltpu.VMEM((rows, coef_count), BF16),
            pltpu.VMEM((coef_count // LANES, rows, LANES), F32),
        ]
        out = jax.ShapeDtypeStruct((rows, coef_count), BF16)
        out_specs, done = vmem, None
        if last and begin < begins[-1]:
            out = jax.ShapeDtypeStruct(piece_shape, BF16)
        elif last:
            out = jax.ShapeDtypeStruct(coeffs.shape, BF16)
            out_specs, done = anywhere, len(earlier)
            scratch += [pltpu.VMEM(piece_shape, BF16), pltpu.SemaphoreType.DMA((len(begins) + 1,))]
            args += earlier
            specs += [vmem] * len(earlier)
        return call(
            functools.partial(
                rest_body,
                (boxes_u, boxes_v, chunk),
                len(levels) if number == 0 else None,
                pairs,
                None if last else after,
                begin,
                done,
            ),
            out,
            scratch,
            product_flops * (1 + 2 * len(pairs)),
            rows * coef_count * 8 + coef_count * coef_count * 2 * (1 + 4 * len(pairs)),
            *args,
            in_specs=specs,
            out_specs=out_specs,
        )

    currents, gots = pieces, raws
    for number, index in enumerate(swaps):
        if number:
            gots = []
            for current in currents:
                gots.append(partner_2(current, levels[index][2], levels[index][3]))
        owns = [own_part(number, current) for current in currents]
        following = []
        for own, got, begin in zip(owns, gots, begins):
            following.append(rest_part(number, own, got, begin, following))
        currents = following
    return currents[-1]


def solution(mesh):
    in_specs = (
        P(None, ("groups", "ill"), "src", "tgt", None),
        P(None, ("groups", "src"), "tgt", None),
        P(),
        P(),
    )
    out_specs = P(None, ("groups", "ill"), "src", "tgt", None)

    return jax.shard_map(on_device, mesh=mesh, in_specs=in_specs, out_specs=out_specs, check_vma=False)
```
